32 devices in a mesh: row: 4 (over x, core), col: 8 (over z, y).
Axes of the slice: x: 2, y: 2, z: 4, core: 2. Of those that a mesh axis runs over, the one named last changes fastest.
Arguments:
- rhs: float32 [32, 262144], P(None, ('row', 'col')), may hold values from -12.5 to 12.5
- near_blocks: bfloat16 [4096, 4, 4096], P(('row', 'col')), may hold values from -0.1875 to 0.1875
- near_offsets: int32 [4096, 4], P(('row', 'col')), may hold values from -4 to 4, as said below
- v_factor: bfloat16 [4096, 2048], P(('row', 'col')), may hold values from -0.75 to 0.75
- mix_col: bfloat16 [4, 128, 256, 256], P('row', 'col'), may hold values from -0.375 to 0.375
- mix_row: bfloat16 [16, 64, 128, 128], P('row', 'col'), may hold values from -0.5 to 0.5
- u_factor: bfloat16 [4096, 2048], P(('row', 'col')), may hold values from -0.75 to 0.75
Outputs:
- solution: float32 [32, 262144], P(None, ('row', 'col'))
- residual: float32 [32, 262144], P(None, ('row', 'col'))
The draws below stay inside these ranges and needn't reach their ends.
Inputs may be any that keep to these rules, and one draw needn't show every extreme that they name: `near_offsets`: column 0 is 0; the other entries of a row are distinct and nonzero. In every aligned block of 128 rows some row holds -4 and some row holds 4.
All inputs are finite; a program needn't handle non-finite values.
Results may differ from the reference program's by a relative error of at most 0.0054.
Values may be sent and summed in bfloat16 or wider, within the bound.
A program may use at most 128 MiB of HBM per device.

```python
import jax
import jax.numpy as jnp
from jax import lax

RHS = 32
LEAF = 64
RANK = 32
NNEAR = 4
HALO = 4
LEAVES_DEV = 128
NLEAVES = 4096
N_UNKNOWNS = 262144
SLOTS = 16
SUBSLOTS = 4
N_ROW = 4
N_COL = 8
DEVICES = 32


def draw_rhs(key, part):
    scale_key = jax.random.fold_in(key, 11)
    value_key = jax.random.fold_in(key, 12)
    scales = jnp.exp(jax.random.uniform(scale_key, (DEVICES,), jnp.float32, jnp.log(0.2), jnp.log(2.5)))
    scales = jnp.repeat(scales, N_UNKNOWNS // DEVICES)[None, :]
    values = jnp.clip(jax.random.normal(value_key, (RHS, N_UNKNOWNS), jnp.float32), -5.0, 5.0)
    return (values * scales).astype(jnp.float32)


def draw_near_offsets(key, part):
    score_key = jax.random.fold_in(key, 21)
    choices_count = 2 * HALO
    column = jnp.arange(choices_count, dtype=jnp.int32)
    candidates = jnp.where(column < HALO, column - HALO, column - HALO + 1)
    scores = jax.random.randint(score_key, (NLEAVES, choices_count), 0, 2 ** 20, dtype=jnp.int32) * choices_count + column[None, :]
    leading = (jnp.arange(NLEAVES, dtype=jnp.int32) % LEAVES_DEV == 0)[:, None]
    forced = jnp.where(column == 0, -2, jnp.where(column == choices_count - 1, -1, scores))
    scores = jnp.where(leading, forced, scores)
    order = jnp.argsort(scores, axis=1)
    picked = candidates[order[:, :NNEAR - 1]]
    return jnp.concatenate([jnp.zeros((NLEAVES, 1), jnp.int32), picked.astype(jnp.int32)], axis=1)


def shard_levels(stream_key, dims, shards, low, largest):
    loudness = 1.0
    for axis_at, shards_of in shards:
        draws = jax.random.uniform(jax.random.fold_in(jax.random.fold_in(stream_key, 6), axis_at), (shards_of,), jnp.float32, low / len(shards), largest / len(shards))
        loudness = loudness * jnp.repeat(jnp.exp(draws), dims[axis_at] // shards_of).reshape((-1,) + (1,) * (len(dims) - 1 - axis_at))
    return loudness


def normal_values(rng, shape, scale, most, split=(), held_as=jnp.bfloat16):
    level = shard_levels(rng, shape, split, -0.22, 0.18) if split else 1.0
    values = jax.random.normal(rng, shape, jnp.float32) * scale * level
    return jnp.minimum(jnp.maximum(values, -most), most).astype(held_as)


def setup_inputs(seed: int = 0) -> dict:
    arg_keys = jax.random.split(jax.random.key(seed), 8)
    rhs = draw_rhs(jax.random.fold_in(arg_keys[7], 71), 0)
    near_blocks = normal_values(arg_keys[1], (NLEAVES, NNEAR, LEAF * LEAF), (4 * NNEAR * LEAF) ** -0.5, 0.1875, ((0, 32),))
    near_offsets = draw_near_offsets(jax.random.fold_in(arg_keys[7], 71), 0)
    v_factor = normal_values(arg_keys[3], (NLEAVES, LEAF * RANK), LEAF ** -0.5, 0.75, ((0, 32),))
    mix_col = normal_values(arg_keys[4], (N_ROW, N_COL * SLOTS, N_COL * RANK, N_COL * RANK), (N_COL * RANK) ** -0.5, 0.375, ((0, 4), (1, 8)))
    mix_row = normal_values(arg_keys[5], (N_ROW * SUBSLOTS, N_COL * N_COL, N_ROW * RANK, N_ROW * RANK), (N_ROW * RANK) ** -0.5, 0.5, ((0, 4), (1, 8)))
    u_factor = normal_values(arg_keys[6], (NLEAVES, RANK * LEAF), (2 * RANK) ** -0.5, 0.75, ((0, 32),))
    return {"rhs": rhs, "near_blocks": near_blocks, "near_offsets": near_offsets, "v_factor": v_factor, "mix_col": mix_col, "mix_row": mix_row, "u_factor": u_factor}


def near_term(vector_bf, near_blocks, near_offsets):
    padded = jnp.pad(vector_bf, ((0, 0), (HALO * LEAF, HALO * LEAF)))
    padded = padded.reshape(RHS, NLEAVES + 2 * HALO, LEAF)
    blocks = near_blocks.reshape(DEVICES, LEAVES_DEV, NNEAR, LEAF, LEAF)
    offsets = near_offsets.reshape(DEVICES, LEAVES_DEV, NNEAR)

    def one_block(device):
        position = device * LEAVES_DEV + jnp.arange(LEAVES_DEV, dtype=jnp.int32)[:, None] + offsets[device] + HALO
        picked = padded[:, position, :].astype(jnp.float32)
        return jnp.einsum('slnu,lnvu->slv', picked, blocks[device].astype(jnp.float32))
    result = lax.map(one_block, jnp.arange(DEVICES, dtype=jnp.int32))
    return jnp.transpose(result, (1, 0, 2, 3)).reshape(RHS, N_UNKNOWNS)

def far_term(vector_bf, v_factor, mix_col, mix_row, u_factor):
    width_col = N_COL * RANK
    width_row = N_ROW * RANK
    local = vector_bf.reshape(RHS, NLEAVES, LEAF).astype(jnp.float32)
    factor = v_factor.reshape(NLEAVES, LEAF, RANK).astype(jnp.float32)
    coeffs = jnp.einsum('slu,luk->lsk', local, factor).astype(jnp.bfloat16)
    coeffs = coeffs.reshape(N_ROW, N_COL, N_COL, SLOTS, RHS, RANK)
    first_mix = mix_col.reshape(N_ROW, N_COL, SLOTS, N_COL, RANK, width_col)

    def level_one(rowgrp):
        return jnp.einsum('cgjsk,gjckm->gjsm', coeffs[rowgrp].astype(jnp.float32), first_mix[rowgrp].astype(jnp.float32)).astype(jnp.bfloat16)
    first = lax.map(level_one, jnp.arange(N_ROW, dtype=jnp.int32))
    first = first.reshape(N_ROW, N_COL, N_ROW, SUBSLOTS, RHS, N_COL, RANK)
    second_mix = mix_row.reshape(N_ROW, SUBSLOTS, N_COL, N_COL, N_ROW, RANK, width_row)
    expand = u_factor.reshape(N_ROW, N_COL, SUBSLOTS, N_COL, N_ROW, RANK, LEAF)

    def level_two(target):
        picked = lax.dynamic_index_in_dim(first, target, 2, keepdims=False)
        second = jnp.einsum('rgjspk,jgprkn->gjpsn', picked.astype(jnp.float32), second_mix[target].astype(jnp.float32)).astype(jnp.bfloat16)
        second = second.reshape(N_COL, SUBSLOTS, N_COL, RHS, N_ROW, RANK)
        out = jnp.einsum('gjpsqk,gjpqku->sgjpqu', second.astype(jnp.float32), expand[target].astype(jnp.float32))
        return out.reshape(RHS, N_COL * LEAVES_DEV * LEAF)
    result = lax.map(level_two, jnp.arange(N_ROW, dtype=jnp.int32))
    return jnp.transpose(result, (1, 0, 2)).reshape(RHS, N_UNKNOWNS)

def reference(rhs, near_blocks, near_offsets, v_factor, mix_col, mix_row, u_factor):

    def operator(vector):
        vector_bf = vector.astype(jnp.bfloat16)
        return vector + near_term(vector_bf, near_blocks, near_offsets) + far_term(vector_bf, v_factor, mix_col, mix_row, u_factor)
    rhs_length = jnp.sqrt(lax.optimization_barrier(jnp.sum(rhs * rhs, axis=1)))
    basis_first = rhs / rhs_length[:, None]
    image_first = operator(basis_first)
    h_one_one = lax.optimization_barrier(jnp.sum(basis_first * image_first, axis=1))
    rest_first = image_first - h_one_one[:, None] * basis_first
    h_two_one = jnp.sqrt(lax.optimization_barrier(jnp.sum(rest_first * rest_first, axis=1)))
    basis_second = rest_first / h_two_one[:, None]
    image_second = operator(basis_second)
    h_one_two = lax.optimization_barrier(jnp.sum(basis_first * image_second, axis=1))
    h_two_two = lax.optimization_barrier(jnp.sum(basis_second * image_second, axis=1))
    rest_second = image_second - h_one_two[:, None] * basis_first - h_two_two[:, None] * basis_second
    h_three_two = jnp.sqrt(lax.optimization_barrier(jnp.sum(rest_second * rest_second, axis=1)))
    m_first = h_one_one * h_one_one + h_two_one * h_two_one
    m_cross = h_one_one * h_one_two + h_two_one * h_two_two
    m_second = h_one_two * h_one_two + h_two_two * h_two_two + h_three_two * h_three_two
    determ = m_first * m_second - m_cross * m_cross
    coef_first = rhs_length * (m_second * h_one_one - m_cross * h_one_two) / determ
    coef_second = rhs_length * (m_first * h_one_two - m_cross * h_one_one) / determ
    solution = coef_first[:, None] * basis_first + coef_second[:, None] * basis_second
    residual = rhs - coef_first[:, None] * image_first - coef_second[:, None] * image_second
    return (solution, residual)
```

```python
import jax
import jax.numpy as jnp
from jax import lax
from jax.experimental import pallas as pl
from jax.experimental.pallas import tpu as pltpu
from jax.sharding import PartitionSpec as P

LEAF = 64
RANK = 32
HALO = 4


def reduce_kernel(x_ref, o_ref, buf, send_sem, recv_sem):
    n_row = lax.axis_size("row")
    n_col = lax.axis_size("col")
    total = n_row * n_col
    me = lax.axis_index("row") * n_col + lax.axis_index("col")
    barrier = pltpu.get_barrier_semaphore()

    def peer(step):
        target = lax.rem(me + step, total)
        return (target // n_col, lax.rem(target, n_col))

    def greet(step, carry):
        pl.semaphore_signal(
            barrier, inc=1, device_id=peer(step), device_id_type=pl.DeviceIdType.MESH
        )
        return carry

    lax.fori_loop(1, total, greet, 0)
    pl.semaphore_wait(barrier, total - 1)

    def copy(step):
        return pltpu.make_async_remote_copy(
            src_ref=x_ref,
            dst_ref=buf.at[step],
            send_sem=send_sem.at[step],
            recv_sem=recv_sem.at[step],
            device_id=peer(step),
            device_id_type=pl.DeviceIdType.MESH,
        )

    def send(step, carry):
        copy(step).start()
        return carry

    lax.fori_loop(1, total, send, 0)

    def wait(step, carry):
        copy(step).wait()
        return carry

    lax.fori_loop(1, total, wait, 0)
    buf[0] = x_ref[...]
    acc = buf[lax.rem(me, total)]
    for source in range(1, total):
        acc = acc + buf[lax.rem(me + total - source, total)]
    o_ref[...] = acc


def all_sum(rows, call):
    count, width = rows.shape
    total = lax.axis_size("row") * lax.axis_size("col")
    padded = jnp.pad(rows, ((0, 8 - count), (0, 128 - width)))
    out = pl.pallas_call(
        reduce_kernel,
        out_shape=jax.ShapeDtypeStruct((8, 128), jnp.float32),
        in_specs=[pl.BlockSpec(memory_space=pltpu.VMEM)],
        out_specs=pl.BlockSpec(memory_space=pltpu.VMEM),
        scratch_shapes=[
            pltpu.VMEM((total, 8, 128), jnp.float32),
            pltpu.SemaphoreType.DMA((total,)),
            pltpu.SemaphoreType.DMA((total,)),
        ],
        compiler_params=pltpu.CompilerParams(collective_id=call, has_side_effects=True),
        name=f"all_sum_{call}",
    )(padded)
    return out[:count, :width]


def with_halo(block, sides, width):
    for axis, dim in sides:
        count = lax.axis_size(axis)
        forward = [(i, i + 1) for i in range(count - 1)]
        backward = [(target, source) for source, target in forward]
        low = lax.ppermute(
            lax.slice_in_dim(block, block.shape[dim] - width, None, axis=dim), axis, forward
        )
        high = lax.ppermute(lax.slice_in_dim(block, 0, width, axis=dim), axis, backward)
        block = jnp.concatenate([low, block, high], axis=dim)
    return block


def near_part(vector_bf, near_blocks, near_offsets):
    count_rhs = vector_bf.shape[0]
    leaves = near_offsets.shape[0]
    blocks_per = near_offsets.shape[1]
    padded = with_halo(vector_bf, ((("row", "col"), 1),), HALO * LEAF)
    padded = padded.reshape(count_rhs, leaves + 2 * HALO, LEAF)
    position = jnp.arange(leaves, dtype=jnp.int32)[:, None] + near_offsets + HALO
    picked = padded[:, position, :]
    blocks = near_blocks.reshape(leaves, blocks_per, LEAF, LEAF)
    result = jnp.einsum("slnu,lnvu->slv", picked, blocks, preferred_element_type=jnp.float32)
    return result.reshape(count_rhs, leaves * LEAF)


def far_part(vector_bf, v_factor, mix_col, mix_row, u_factor):
    count_rhs = vector_bf.shape[0]
    n_row = lax.axis_size("row")
    n_col = lax.axis_size("col")
    leaves = v_factor.shape[0]
    slots = leaves // n_col
    subslots = slots // n_row
    width_col = n_col * RANK
    width_row = n_row * RANK
    local = vector_bf.reshape(count_rhs, leaves, LEAF)
    coeffs = jnp.einsum(
        "slu,luk->lsk",
        local,
        v_factor.reshape(leaves, LEAF, RANK),
        preferred_element_type=jnp.float32,
    ).astype(jnp.bfloat16)
    grouped = coeffs.reshape(n_col, slots, count_rhs * RANK)
    received = lax.all_to_all(grouped, "col", split_axis=0, concat_axis=0, tiled=True)
    first = jnp.einsum(
        "cjsk,jckm->jsm",
        received.reshape(n_col, slots, count_rhs, RANK),
        mix_col.reshape(slots, n_col, RANK, width_col),
        preferred_element_type=jnp.float32,
    )
    first = first.astype(jnp.bfloat16)
    regrouped = lax.all_to_all(first, "row", split_axis=0, concat_axis=0, tiled=True)
    regrouped = regrouped.reshape(n_row, subslots, count_rhs, n_col, RANK)
    second = jnp.einsum(
        "rjspk,jprkn->jpsn",
        regrouped,
        mix_row.reshape(subslots, n_col, n_row, RANK, width_row),
        preferred_element_type=jnp.float32,
    ).astype(jnp.bfloat16)
    second = second.reshape(subslots, n_col, count_rhs, n_row, RANK)
    expanded = jnp.einsum(
        "jpsqk,jpqku->sjpqu",
        second,
        u_factor.reshape(subslots, n_col, n_row, RANK, LEAF),
        preferred_element_type=jnp.float32,
    )
    return expanded.reshape(count_rhs, leaves * LEAF)


def orthogonal(bases, image, call):
    partial_sums = [jnp.sum(basis * image, axis=1) for basis in bases] + [
        jnp.sum(image * image, axis=1)
    ]
    joined = all_sum(jnp.stack(partial_sums), call)
    sums = joined[:-1]
    rest = image
    for index_basis in range(len(bases)):
        rest = rest - sums[index_basis][:, None] * bases[index_basis]
    length = jnp.sqrt(joined[-1] - jnp.sum(sums * sums, axis=0))
    return (sums, rest, length)


def body(rhs, near_blocks, near_offsets, v_factor, mix_col, mix_row, u_factor):

    def operator(vector):
        vector_bf = vector.astype(jnp.bfloat16)
        return (
            vector
            + near_part(vector_bf, near_blocks, near_offsets)
            + far_part(vector_bf, v_factor, mix_col, mix_row, u_factor)
        )

    rhs_length = jnp.sqrt(all_sum(jnp.sum(rhs * rhs, axis=1)[None], 0)[0])
    basis_first = rhs / rhs_length[:, None]
    image_first = operator(basis_first)
    proj_first, rest_first, h_two_one = orthogonal((basis_first,), image_first, 1)
    h_one_one = proj_first[0]
    basis_second = rest_first / h_two_one[:, None]
    image_second = operator(basis_second)
    proj_second, rest_second, h_three_two = orthogonal((basis_first, basis_second), image_second, 2)
    h_one_two = proj_second[0]
    h_two_two = proj_second[1]
    m_first = h_one_one * h_one_one + h_two_one * h_two_one
    m_cross = h_one_one * h_one_two + h_two_one * h_two_two
    m_second = h_one_two * h_one_two + h_two_two * h_two_two + h_three_two * h_three_two
    determ = m_first * m_second - m_cross * m_cross
    coef_first = rhs_length * (m_second * h_one_one - m_cross * h_one_two) / determ
    coef_second = rhs_length * (m_first * h_one_two - m_cross * h_one_one) / determ
    solution = coef_first[:, None] * basis_first + coef_second[:, None] * basis_second
    residual = rhs - coef_first[:, None] * image_first - coef_second[:, None] * image_second
    return (solution, residual)


def solution(mesh):
    in_specs = (
        P(None, ("row", "col")),
        P(("row", "col"), None, None),
        P(("row", "col"), None),
        P(("row", "col"), None),
        P("row", "col", None, None),
        P("row", "col", None, None),
        P(("row", "col"), None),
    )
    out_specs = (P(None, ("row", "col")), P(None, ("row", "col")))
    return jax.shard_map(body, mesh=mesh, in_specs=in_specs, out_specs=out_specs, check_vma=False)
```

```python
import jax
import jax.numpy as jnp
from jax import lax
from jax.experimental import pallas as pl
from jax.experimental.pallas import tpu as pltpu
from jax.sharding import PartitionSpec as P

LEAF = 64
RANK = 32
HALO = 4
LANES = 128
QUAD = LANES // RANK
BF16 = jnp.bfloat16
F32 = jnp.float32
MESH = pl.DeviceIdType.MESH


def iota(shape, dim):
    return lax.broadcasted_iota(jnp.int32, shape, dim)


def dot(a, b):
    return jnp.dot(a, b, preferred_element_type=F32)


def lanes_at(index, width):
    return pl.ds(pl.multiple_of(index * width, width), width)


def regroup(tiles, group):
    out = []
    for j in range(QUAD):
        made = None
        for c in range(QUAD):
            shift = (c - j) * RANK % LANES
            moved = pltpu.roll(tiles[c], shift, 1) if shift else tiles[c]
            made = moved if made is None else jnp.where(group == c, moved, made)
        out.append(made)
    return out


def kernel(
    offs, rhs_h, near_h, v_h, mixc_h, mixr_h, u_h, sol, res,
    rhs, near_raw, v_raw, mixc, mixr, u_raw,
    near_w, v_big, u_big, pick_near, pick_v, pick_u,
    xbf, xdup, w_one, w_two, q_two,
    zbuf, zrecv, tbuf, trecv, halo, part, sum_c, sum_r,
    load_sem, halo_s, halo_r, z_s, z_r, t_s, t_r, c_s, c_r, r_s, r_r,
):
    n_row = lax.axis_size("row")
    n_col = lax.axis_size("col")
    total = n_row * n_col
    row = lax.axis_index("row")
    col = lax.axis_index("col")
    me = row * n_col + col
    count, width = rhs.shape
    leaves = width // LEAF
    nnear = offs.shape[1]
    slots = leaves // n_col
    sub = slots // n_row
    edge = HALO * LEAF

    loads = {}
    for at, (name, src, dst) in enumerate(
        (("v", v_h, v_raw), ("rhs", rhs_h, rhs), ("near", near_h, near_raw),
         ("mixc", mixc_h, mixc), ("mixr", mixr_h, mixr), ("u", u_h, u_raw))
    ):
        loads[name] = pltpu.make_async_copy(src, dst, load_sem.at[at])
        loads[name].start()

    barrier = pltpu.get_barrier_semaphore()
    before = lax.rem(me + total - 1, total)
    after = lax.rem(me + 1, total)
    before_id = (before // n_col, lax.rem(before, n_col))
    after_id = (after // n_col, lax.rem(after, n_col))

    def col_id(step):
        return (row, lax.rem(col + step, n_col))

    def row_id(step):
        return (lax.rem(row + step, n_row), col)

    for step in range(1, n_col):
        pl.semaphore_signal(barrier, inc=1, device_id=col_id(step), device_id_type=MESH)
    for step in range(1, n_row):
        pl.semaphore_signal(barrier, inc=1, device_id=row_id(step), device_id_type=MESH)
    pl.semaphore_signal(barrier, inc=1, device_id=before_id, device_id_type=MESH)
    pl.semaphore_signal(barrier, inc=1, device_id=after_id, device_id_type=MESH)

    lane = iota((count, LANES), 1)
    low = lane < LEAF
    group = lane // RANK

    r = iota(pick_v.shape, 0)
    c = iota(pick_v.shape, 1)
    pick_v[...] = jnp.where((c % 16 == r // LEAF) & (c // 16 == r % LEAF // QUAD), 1.0, 0.0).astype(BF16)
    r = iota(pick_u.shape, 0)
    c = iota(pick_u.shape, 1)
    pick_u[...] = jnp.where((c % 16 == r // RANK) & (c // 16 == r % RANK // 2), 1.0, 0.0).astype(BF16)
    r = iota(pick_near.shape, 0)
    c = iota(pick_near.shape, 1)
    pick_near[...] = jnp.where((c % nnear == r // LEAF) & (c // nnear == r % LEAF // 2), 1.0, 0.0).astype(BF16)

    def prepare_v():
        loads["v"].wait()
        rr = iota((QUAD * LEAF, LANES), 0)
        gg = iota((QUAD * LEAF, LANES), 1) // RANK
        own = gg == rr % QUAD
        place = gg == rr // LEAF

        def block(b, carry):
            base = pl.multiple_of(b * 16, 16)
            rows = jnp.concatenate(
                [v_raw[pl.ds(base, 16), t * LANES:(t + 1) * LANES] for t in range(16)], axis=0
            )
            for q in range(4):
                size = QUAD * LEAF
                m = dot(pick_v[q * size:(q + 1) * size, :], rows)
                m = jnp.where(own, m, 0.0)
                m = m + pltpu.roll(m, RANK, 1)
                m = m + pltpu.roll(m, 2 * RANK, 1)
                at = pl.multiple_of(b * 16 * LEAF + q * size, size)
                v_big[pl.ds(at, size), :] = jnp.where(place, m, 0.0).astype(BF16)
            return carry

        lax.fori_loop(0, leaves // 16, block, 0)

    def prepare_u():
        loads["u"].wait()
        size = QUAD * RANK
        rr = iota((size, LANES), 0)
        half = iota((size, LANES), 1) // LEAF
        own = half == rr % 2
        place = (rr // RANK) - half

        def block(b, carry):
            base = pl.multiple_of(b * 16, 16)
            rows = jnp.concatenate(
                [u_raw[pl.ds(base, 16), t * LANES:(t + 1) * LANES] for t in range(16)], axis=0
            )
            for q in range(4):
                m = dot(pick_u[q * size:(q + 1) * size, :], rows)
                m = jnp.where(own, m, 0.0)
                m = m + pltpu.roll(m, LEAF, 1)
                at = pl.multiple_of(b * 16 * RANK + q * size, size)
                u_big[pl.ds(at, size), 0:LANES] = jnp.where(place == 0, m, 0.0).astype(BF16)
                u_big[pl.ds(at, size), LANES:2 * LANES] = jnp.where(place == 2, m, 0.0).astype(BF16)
            return carry

        lax.fori_loop(0, leaves // 16, block, 0)

    def prepare_near():
        loads["near"].wait()
        rr = iota((LEAF, LANES), 0)
        left = iota((LEAF, LANES), 1) < LEAF
        own = left == (rr % 2 == 0)
        size = nnear * LEAF // 2

        def block(b, carry):
            for k in range(2):
                leaf = b * 2 + k
                m = dot(pick_near[...], near_raw[lanes_at(leaf, size), :])
                for pair in range(nnear // 2):
                    a = jnp.where(own, m[2 * pair * LEAF:(2 * pair + 1) * LEAF], 0.0)
                    d = jnp.where(own, m[(2 * pair + 1) * LEAF:(2 * pair + 2) * LEAF], 0.0)
                    made = jnp.where(left, a, d) + pltpu.roll(jnp.where(left, d, a), LEAF, 1)
                    near_w[lanes_at(leaf, LEAF), pair * LANES:(pair + 1) * LANES] = made.astype(BF16)
            return carry

        lax.fori_loop(0, leaves // 2, block, 0)

    def spread(tile, first):
        turned = pltpu.roll(tile, LEAF, 1)
        xdup[first] = jnp.where(low, tile, turned).astype(BF16)
        xdup[first + 1] = jnp.where(low, turned, tile).astype(BF16)

    def remote(src, dst, send, recv, to):
        return pltpu.make_async_remote_copy(
            src_ref=src, dst_ref=dst, send_sem=send, recv_sem=recv, device_id=to, device_id_type=MESH
        )

    def all_sum(at, rows):
        eye = iota((count, LANES), 0) == lane
        pick = iota((8, LANES), 0)
        tile = jnp.zeros((8, LANES), F32)
        for k, acc in enumerate(rows):
            line = jnp.sum(jnp.where(eye, jnp.sum(acc, axis=1, keepdims=True), 0.0), axis=0, keepdims=True)
            tile = jnp.where(pick == k, line, tile)
        for slot, n, here, buf, send, recv, ids in (
            (0, n_col, col, sum_c, c_s, c_r, col_id), (1, n_row, row, sum_r, r_s, r_r, row_id)
        ):
            part[at, slot] = tile
            buf[at, 0] = tile
            copies = [
                remote(part.at[at, slot], buf.at[at, s], send.at[at, s], recv.at[at, s], ids(s))
                for s in range(1, n)
            ]
            for copy in copies:
                copy.start()
            for copy in copies:
                copy.wait()
            tile = buf[at, here]
            for source in range(1, n):
                tile = tile + buf[at, lax.rem(here + n - source, n)]
        return [
            jnp.sum(jnp.where(eye, tile[k:k + 1, :], 0.0), axis=1, keepdims=True) for k in range(len(rows))
        ]

    def operator(at, x, w, others):
        h_low = remote(xbf.at[:, width - edge:width], halo.at[at, 0], halo_s.at[at, 0], halo_r.at[at, 0], after_id)
        h_high = remote(xbf.at[:, 0:edge], halo.at[at, 1], halo_s.at[at, 1], halo_r.at[at, 1], before_id)
        h_low.start()
        h_high.start()
        tiles = slots // QUAD
        for g4 in range(leaves // QUAD):
            z = dot(xbf[:, g4 * 256:(g4 + 1) * 256], v_big[g4 * 256:(g4 + 1) * 256, :])
            zbuf[g4 // tiles, :, g4 % tiles * LANES:(g4 % tiles + 1) * LANES] = z.astype(BF16)
        z_copies = []
        for s in range(1, n_col):
            z_copies.append(
                remote(zbuf.at[lax.rem(col + s, n_col)], zrecv.at[at, s], z_s.at[at, s], z_r.at[at, s], col_id(s))
            )
            z_copies[-1].start()
        zrecv[at, 0] = zbuf[col]
        if at == 0:
            prepare_near()
        h_low.wait()
        h_high.wait()
        for side, beyond, first in ((0, me == 0, 0), (1, me == total - 1, leaves + HALO)):
            for k in range(HALO // 2):
                tile = halo[at, side, :, k * LANES:(k + 1) * LANES].astype(F32)
                spread(jnp.where(beyond, 0.0, tile), first + 2 * k)

        def near(b, carry):
            for pair in range(4):
                outs = []
                for k in range(2):
                    leaf = b * 8 + pair * 2 + k
                    picked = [xdup[leaf + HALO + offs[leaf, n]] for n in range(nnear)]
                    left = jnp.concatenate(
                        [jnp.where(low, picked[2 * m], picked[2 * m + 1]) for m in range(nnear // 2)], axis=1
                    )
                    outs.append(
                        lax.dot_general(
                            left, near_w[lanes_at(leaf, LEAF), :], (((1,), (1,)), ((), ())),
                            preferred_element_type=F32,
                        )
                    )
                where = lanes_at(b * 4 + pair, LANES)
                w[:, where] = x[:, where] + jnp.concatenate(outs, axis=1)
            return carry

        steps = leaves // 8
        lax.fori_loop(0, steps // 2, near, 0)
        for copy in z_copies:
            copy.wait()
        if at == 0:
            loads["mixc"].wait()
        for jt in range(tiles):
            lefts = [[] for _ in range(QUAD)]
            for cq in range(n_col // QUAD):
                got = regroup(
                    [
                        zrecv[at, lax.rem(col + n_col - (cq * QUAD + c4), n_col), :, jt * LANES:(jt + 1) * LANES].astype(F32)
                        for c4 in range(QUAD)
                    ],
                    group,
                )
                for j4 in range(QUAD):
                    lefts[j4].append(got[j4].astype(BF16))
            for j4 in range(QUAD):
                j = jt * QUAD + j4
                first = dot(jnp.concatenate(lefts[j4], axis=1), mixc[j])
                tbuf[j // sub, j % sub] = first.astype(BF16)
        t_copies = []
        for s in range(1, n_row):
            t_copies.append(
                remote(tbuf.at[lax.rem(row + s, n_row)], trecv.at[at, s], t_s.at[at, s], t_r.at[at, s], row_id(s))
            )
            t_copies[-1].start()
        trecv[at, 0] = tbuf[row]
        if at == 0:
            prepare_u()
        lax.fori_loop(steps // 2, steps, near, 0)
        for copy in t_copies:
            copy.wait()
        if at == 0:
            loads["mixr"].wait()
        sums = [jnp.zeros((count, LANES), F32) for _ in range(len(others) + 1)]
        for i in range(sub):
            for pq in range(n_col // QUAD):
                lefts = [[] for _ in range(QUAD)]
                for rq in range(n_row // QUAD):
                    got = regroup(
                        [
                            trecv[at, lax.rem(row + n_row - (rq * QUAD + r4), n_row), i, :, pq * LANES:(pq + 1) * LANES].astype(F32)
                            for r4 in range(QUAD)
                        ],
                        group,
                    )
                    for p4 in range(QUAD):
                        lefts[p4].append(got[p4].astype(BF16))
                for p4 in range(QUAD):
                    p = pq * QUAD + p4
                    second = dot(jnp.concatenate(lefts[p4], axis=1), mixr[i, p]).astype(BF16)
                    for tt in range(n_row // QUAD):
                        at4 = (i * n_col + p) * (n_row // QUAD) + tt
                        far = dot(second[:, tt * LANES:(tt + 1) * LANES], u_big[at4 * LANES:(at4 + 1) * LANES, :])
                        for k in range(2):
                            where = slice(at4 * 256 + k * LANES, at4 * 256 + (k + 1) * LANES)
                            image = w[:, where] + far[:, k * LANES:(k + 1) * LANES]
                            w[:, where] = image
                            for m, other in enumerate(others):
                                sums[m] = sums[m] + other[:, where] * image
                            sums[-1] = sums[-1] + image * image
        return sums

    prepare_v()
    loads["rhs"].wait()

    def start_tile(t, acc):
        where = lanes_at(t, LANES)
        tile = rhs[:, where]
        xbf[:, where] = tile.astype(BF16)
        spread(tile, HALO + 2 * t)
        return acc + tile * tile

    norm = lax.fori_loop(0, width // LANES, start_tile, jnp.zeros((count, LANES), F32))
    pl.semaphore_wait(barrier, n_col + n_row)
    first = operator(0, rhs, w_one, (rhs,))
    norm_sq, cross, image_sq = all_sum(0, [norm] + first)
    beta = jnp.sqrt(norm_sq)
    h11 = cross / norm_sq
    h21 = jnp.sqrt(image_sq / norm_sq - h11 * h11)
    scale = 1.0 / (beta * h21)

    def second_tile(t, carry):
        where = lanes_at(t, LANES)
        tile = (w_one[:, where] - h11 * rhs[:, where]) * scale
        q_two[:, where] = tile
        xbf[:, where] = tile.astype(BF16)
        spread(tile, HALO + 2 * t)
        return carry

    lax.fori_loop(0, width // LANES, second_tile, 0)
    second = operator(1, q_two, w_two, (rhs, q_two))
    with_first, h22, image_sq = all_sum(1, second)
    h12 = with_first / beta
    h32 = jnp.sqrt(image_sq - (h12 * h12 + h22 * h22))
    m11 = h11 * h11 + h21 * h21
    m12 = h11 * h12 + h21 * h22
    m22 = h12 * h12 + h22 * h22 + h32 * h32
    det = m11 * m22 - m12 * m12
    y1 = (m22 * h11 - m12 * h12) / det
    y2 = beta * (m11 * h12 - m12 * h11) / det

    def last_tile(t, carry):
        where = lanes_at(t, LANES)
        sol[:, where] = y1 * rhs[:, where] + y2 * q_two[:, where]
        res[:, where] = rhs[:, where] - y1 * w_one[:, where] - y2 * w_two[:, where]
        return carry

    lax.fori_loop(0, width // LANES, last_tile, 0)


def body(rhs, near_blocks, near_offsets, v_factor, mix_col, mix_row, u_factor):
    n_row = lax.axis_size("row")
    n_col = lax.axis_size("col")
    count, width = rhs.shape
    leaves, nnear = near_offsets.shape
    pieces = near_blocks.shape[2] // LANES
    near_rows = (
        near_blocks.reshape(leaves, nnear, pieces, LANES).transpose(0, 2, 1, 3).reshape(leaves * pieces * nnear, LANES)
    )
    mixc = mix_col[0]
    slots = leaves // n_col
    sub = slots // n_row
    vmem = pltpu.VMEM
    dma = pltpu.SemaphoreType.DMA
    field = vmem((count, width), F32)
    any_spec = pl.BlockSpec(memory_space=pl.ANY)
    return pl.pallas_call(
        kernel,
        out_shape=(jax.ShapeDtypeStruct((count, width), F32),) * 2,
        in_specs=[pl.BlockSpec(memory_space=pltpu.SMEM)] + [any_spec] * 6,
        out_specs=(pl.BlockSpec(memory_space=pltpu.VMEM),) * 2,
        scratch_shapes=[
            field,
            vmem(near_rows.shape, BF16),
            vmem(v_factor.shape, BF16),
            vmem(mixc.shape, BF16),
            vmem(mix_row.shape, BF16),
            vmem(u_factor.shape, BF16),
            vmem((leaves * LEAF, nnear * LEAF), BF16),
            vmem((leaves * LEAF, LANES), BF16),
            vmem((leaves * RANK, 2 * LANES), BF16),
            vmem((nnear * LEAF, pieces * nnear), BF16),
            vmem((16 * LEAF, 256), BF16),
            vmem((16 * RANK, 256), BF16),
            vmem((count, width), BF16),
            vmem((leaves + 2 * HALO, count, LANES), BF16),
            field,
            field,
            field,
            vmem((n_col, count, slots * RANK), BF16),
            vmem((2, n_col, count, slots * RANK), BF16),
            vmem((n_row, sub, count, n_col * RANK), BF16),
            vmem((2, n_row, sub, count, n_col * RANK), BF16),
            vmem((2, 2, count, HALO * LEAF), BF16),
            vmem((2, 2, 8, LANES), F32),
            vmem((2, n_col, 8, LANES), F32),
            vmem((2, n_row, 8, LANES), F32),
            dma((6,)),
            dma((2, 2)),
            dma((2, 2)),
            dma((2, n_col)),
            dma((2, n_col)),
            dma((2, n_row)),
            dma((2, n_row)),
            dma((2, n_col)),
            dma((2, n_col)),
            dma((2, n_row)),
            dma((2, n_row)),
        ],
        compiler_params=pltpu.CompilerParams(
            collective_id=0, has_side_effects=True, vmem_limit_bytes=60 * 1024 * 1024
        ),
        name="gmres",
    )(near_offsets, rhs, near_rows, v_factor, mixc, mix_row, u_factor)


def solution(mesh):
    in_specs = (
        P(None, ("row", "col")),
        P(("row", "col"), None, None),
        P(("row", "col"), None),
        P(("row", "col"), None),
        P("row", "col", None, None),
        P("row", "col", None, None),
        P(("row", "col"), None),
    )
    out_specs = (P(None, ("row", "col")), P(None, ("row", "col")))
    return jax.shard_map(body, mesh=mesh, in_specs=in_specs, out_specs=out_specs, check_vma=False)
```

```python
import jax
import jax.numpy as jnp
from jax import lax
from jax.experimental import pallas as pl
from jax.experimental.pallas import tpu as pltpu
from jax.sharding import PartitionSpec as P

LEAF = 64
RANK = 32
HALO = 4
LANES = 128
QUAD = LANES // RANK
BF16 = jnp.bfloat16
F32 = jnp.float32
MESH = pl.DeviceIdType.MESH


def iota(shape, dim):
    return lax.broadcasted_iota(jnp.int32, shape, dim)


def dot(a, b):
    return jnp.dot(a, b, preferred_element_type=F32)


def lanes_at(index, width):
    return pl.ds(pl.multiple_of(index * width, width), width)


def regroup(tiles, group):
    out = []
    for j in range(QUAD):
        made = None
        for c in range(QUAD):
            shift = (c - j) * RANK % LANES
            moved = pltpu.roll(tiles[c], shift, 1) if shift else tiles[c]
            made = moved if made is None else jnp.where(group == c, moved, made)
        out.append(made)
    return out


def kernel(
    offs, rhs_h, near_h, v_h, mixc_h, mixr_h, u_h, sol, res,
    rhs, near_raw, v_raw, mixc, mixr, u_raw,
    near_w, v_big, u_big, pick_near, pick_v, pick_u,
    xbf, xdup, w_one, w_two, q_two,
    zbuf, zrecv, tbuf, trecv, halo, part, sums,
    load_sem, halo_s, halo_r, z_s, z_r, t_s, t_r, sum_s, sum_r,
):
    n_row = lax.axis_size("row")
    n_col = lax.axis_size("col")
    total = n_row * n_col
    row = lax.axis_index("row")
    col = lax.axis_index("col")
    me = row * n_col + col
    count, width = rhs.shape
    leaves = width // LEAF
    nnear = offs.shape[1]
    slots = leaves // n_col
    sub = slots // n_row
    edge = HALO * LEAF

    loads = {}
    for at, (name, src, dst) in enumerate(
        (("v", v_h, v_raw), ("rhs", rhs_h, rhs), ("near", near_h, near_raw),
         ("mixc", mixc_h, mixc), ("mixr", mixr_h, mixr), ("u", u_h, u_raw))
    ):
        loads[name] = pltpu.make_async_copy(src, dst, load_sem.at[at])
        if name in ("v", "rhs"):
            loads[name].start()

    barrier = pltpu.get_barrier_semaphore()
    before = lax.rem(me + total - 1, total)
    after = lax.rem(me + 1, total)
    before_id = (before // n_col, lax.rem(before, n_col))
    after_id = (after // n_col, lax.rem(after, n_col))

    def col_id(step):
        return (row, lax.rem(col + step, n_col))

    def row_id(step):
        return (lax.rem(row + step, n_row), col)

    def any_id(step):
        other = lax.rem(me + step, total)
        return (other // n_col, lax.rem(other, n_col))

    def greet(step, carry):
        pl.semaphore_signal(barrier, inc=1, device_id=any_id(step), device_id_type=MESH)
        return carry

    lax.fori_loop(1, total, greet, 0)

    lane = iota((count, LANES), 1)
    low = lane < LEAF
    group = lane // RANK

    r = iota(pick_v.shape, 0)
    c = iota(pick_v.shape, 1)
    pick_v[...] = jnp.where((c % 16 == r // LEAF) & (c // 16 == r % LEAF // QUAD), 1.0, 0.0).astype(BF16)
    r = iota(pick_u.shape, 0)
    c = iota(pick_u.shape, 1)
    pick_u[...] = jnp.where((c % 16 == r // RANK) & (c // 16 == r % RANK // 2), 1.0, 0.0).astype(BF16)
    r = iota(pick_near.shape, 0)
    c = iota(pick_near.shape, 1)
    pick_near[...] = jnp.where((c % nnear == r // LEAF) & (c // nnear == r % LEAF // 2), 1.0, 0.0).astype(BF16)

    def prepare_v():
        loads["v"].wait()
        for name in ("near", "mixc", "mixr", "u"):
            loads[name].start()
        rr = iota((QUAD * LEAF, LANES), 0)
        gg = iota((QUAD * LEAF, LANES), 1) // RANK
        own = gg == rr % QUAD
        place = gg == rr // LEAF

        def block(b, carry):
            base = pl.multiple_of(b * 16, 16)
            rows = jnp.concatenate(
                [v_raw[pl.ds(base, 16), t * LANES:(t + 1) * LANES] for t in range(16)], axis=0
            )
            for q in range(4):
                size = QUAD * LEAF
                m = dot(pick_v[q * size:(q + 1) * size, :], rows)
                m = jnp.where(own, m, 0.0)
                m = m + pltpu.roll(m, RANK, 1)
                m = m + pltpu.roll(m, 2 * RANK, 1)
                at = pl.multiple_of(b * 16 * LEAF + q * size, size)
                v_big[pl.ds(at, size), :] = jnp.where(place, m, 0.0).astype(BF16)
            return carry

        lax.fori_loop(0, leaves // 16, block, 0)

    def prepare_u():
        loads["u"].wait()
        size = QUAD * RANK
        rr = iota((size, LANES), 0)
        half = iota((size, LANES), 1) // LEAF
        own = half == rr % 2
        place = (rr // RANK) - half

        def block(b, carry):
            base = pl.multiple_of(b * 16, 16)
            rows = jnp.concatenate(
                [u_raw[pl.ds(base, 16), t * LANES:(t + 1) * LANES] for t in range(16)], axis=0
            )
            for q in range(4):
                m = dot(pick_u[q * size:(q + 1) * size, :], rows)
                m = jnp.where(own, m, 0.0)
                m = m + pltpu.roll(m, LEAF, 1)
                at = pl.multiple_of(b * 16 * RANK + q * size, size)
                u_big[pl.ds(at, size), 0:LANES] = jnp.where(place == 0, m, 0.0).astype(BF16)
                u_big[pl.ds(at, size), LANES:2 * LANES] = jnp.where(place == 2, m, 0.0).astype(BF16)
            return carry

        lax.fori_loop(0, leaves // 16, block, 0)

    def prepare_near():
        loads["near"].wait()
        rr = iota((LEAF, LANES), 0)
        left = iota((LEAF, LANES), 1) < LEAF
        own = left == (rr % 2 == 0)
        size = nnear * LEAF // 2

        def block(b, carry):
            for k in range(2):
                twin = b * 4 + k * 2
                both = dot(
                    pick_near[...],
                    jnp.concatenate(
                        [near_raw[lanes_at(twin, size), :], near_raw[lanes_at(twin + 1, size), :]], axis=1
                    ),
                )
                for which in range(2):
                    m = both[:, which * LANES:(which + 1) * LANES]
                    for pair in range(nnear // 2):
                        a = m[2 * pair * LEAF:(2 * pair + 1) * LEAF]
                        d = m[(2 * pair + 1) * LEAF:(2 * pair + 2) * LEAF]
                        straight = jnp.where(own, jnp.where(left, a, d), 0.0)
                        crossed = jnp.where(own, jnp.where(left, d, a), 0.0)
                        made = straight + pltpu.roll(crossed, LEAF, 1)
                        near_w[lanes_at(twin + which, LEAF), pair * LANES:(pair + 1) * LANES] = made.astype(BF16)
            return carry

        lax.fori_loop(0, leaves // 4, block, 0)

    def spread(tile, first):
        turned = pltpu.roll(tile, LEAF, 1)
        xdup[first] = jnp.where(low, tile, turned).astype(BF16)
        xdup[first + 1] = jnp.where(low, turned, tile).astype(BF16)

    def remote(src, dst, send, recv, to):
        return pltpu.make_async_remote_copy(
            src_ref=src, dst_ref=dst, send_sem=send, recv_sem=recv, device_id=to, device_id_type=MESH
        )

    def all_sum(at, rows):
        spot = lane - iota((count, LANES), 0)
        spread_out = jnp.zeros((count, LANES), F32)
        for k, acc in enumerate(rows):
            spread_out = jnp.where(spot == k * count, jnp.sum(acc, axis=1, keepdims=True), spread_out)
        line = jnp.sum(spread_out, axis=0, keepdims=True)
        part[at] = line
        sums[at, 0] = line

        def copy(s):
            return remote(part.at[at], sums.at[at, s], sum_s.at[at, s], sum_r.at[at, s], any_id(s))

        def start(s, carry):
            copy(s).start()
            return carry

        def wait(s, carry):
            copy(s).wait()
            return carry

        lax.fori_loop(1, total, start, 0)
        lax.fori_loop(1, total, wait, 0)
        parts = [sums[at, lax.rem(me + total - d, total)] for d in range(total)]
        while len(parts) > 1:
            parts = [parts[i] + parts[i + 1] for i in range(0, len(parts), 2)]
        line = parts[0]
        return [
            jnp.sum(jnp.where(spot == k * count, line, 0.0), axis=1, keepdims=True) for k in range(len(rows))
        ]

    def operator(at, x, w, others):
        h_low = remote(xbf.at[:, width - edge:width], halo.at[at, 0], halo_s.at[at, 0], halo_r.at[at, 0], after_id)
        h_high = remote(xbf.at[:, 0:edge], halo.at[at, 1], halo_s.at[at, 1], halo_r.at[at, 1], before_id)
        h_low.start()
        h_high.start()
        tiles = slots // QUAD
        for g4 in range(leaves // QUAD):
            z = dot(xbf[:, g4 * 256:(g4 + 1) * 256], v_big[g4 * 256:(g4 + 1) * 256, :])
            zbuf[g4 // tiles, :, g4 % tiles * LANES:(g4 % tiles + 1) * LANES] = z.astype(BF16)
        z_copies = []
        for s in range(1, n_col):
            z_copies.append(
                remote(zbuf.at[lax.rem(col + s, n_col)], zrecv.at[at, s], z_s.at[at, s], z_r.at[at, s], col_id(s))
            )
            z_copies[-1].start()
        zrecv[at, 0] = zbuf[col]
        if at == 0:
            prepare_near()
        h_low.wait()
        h_high.wait()
        for side, beyond, first in ((0, me == 0, 0), (1, me == total - 1, leaves + HALO)):
            for k in range(HALO // 2):
                tile = halo[at, side, :, k * LANES:(k + 1) * LANES].astype(F32)
                spread(jnp.where(beyond, 0.0, tile), first + 2 * k)

        def near(b, carry):
            for pair in range(4):
                outs = []
                for k in range(2):
                    leaf = b * 8 + pair * 2 + k
                    picked = [xdup[leaf + HALO + offs[leaf, n]] for n in range(nnear)]
                    left = jnp.concatenate(
                        [jnp.where(low, picked[2 * m], picked[2 * m + 1]) for m in range(nnear // 2)], axis=1
                    )
                    outs.append(
                        lax.dot_general(
                            left, near_w[lanes_at(leaf, LEAF), :], (((1,), (1,)), ((), ())),
                            preferred_element_type=F32,
                        )
                    )
                where = lanes_at(b * 4 + pair, LANES)
                w[:, where] = x[:, where] + jnp.concatenate(outs, axis=1)
            return carry

        steps = leaves // 8
        lax.fori_loop(0, steps // 2, near, 0)
        for copy in z_copies:
            copy.wait()
        if at == 0:
            loads["mixc"].wait()
        for jt in range(tiles):
            lefts = [[] for _ in range(QUAD)]
            for cq in range(n_col // QUAD):
                got = regroup(
                    [
                        zrecv[at, lax.rem(col + n_col - (cq * QUAD + c4), n_col), :, jt * LANES:(jt + 1) * LANES].astype(F32)
                        for c4 in range(QUAD)
                    ],
                    group,
                )
                for j4 in range(QUAD):
                    lefts[j4].append(got[j4].astype(BF16))
            for j4 in range(QUAD):
                j = jt * QUAD + j4
                first = dot(jnp.concatenate(lefts[j4], axis=1), mixc[j])
                tbuf[j // sub, j % sub] = first.astype(BF16)
        t_copies = []
        for s in range(1, n_row):
            t_copies.append(
                remote(tbuf.at[lax.rem(row + s, n_row)], trecv.at[at, s], t_s.at[at, s], t_r.at[at, s], row_id(s))
            )
            t_copies[-1].start()
        trecv[at, 0] = tbuf[row]
        if at == 0:
            prepare_u()
        lax.fori_loop(steps // 2, steps, near, 0)
        for copy in t_copies:
            copy.wait()
        if at == 0:
            loads["mixr"].wait()
        accs = [jnp.zeros((count, LANES), F32) for _ in range(len(others) + 1)]
        for i in range(sub):
            for pq in range(n_col // QUAD):
                lefts = [[] for _ in range(QUAD)]
                for rq in range(n_row // QUAD):
                    got = regroup(
                        [
                            trecv[at, lax.rem(row + n_row - (rq * QUAD + r4), n_row), i, :, pq * LANES:(pq + 1) * LANES].astype(F32)
                            for r4 in range(QUAD)
                        ],
                        group,
                    )
                    for p4 in range(QUAD):
                        lefts[p4].append(got[p4].astype(BF16))
                for p4 in range(QUAD):
                    p = pq * QUAD + p4
                    second = dot(jnp.concatenate(lefts[p4], axis=1), mixr[i, p]).astype(BF16)
                    for tt in range(n_row // QUAD):
                        at4 = (i * n_col + p) * (n_row // QUAD) + tt
                        far = dot(second[:, tt * LANES:(tt + 1) * LANES], u_big[at4 * LANES:(at4 + 1) * LANES, :])
                        for k in range(2):
                            where = slice(at4 * 256 + k * LANES, at4 * 256 + (k + 1) * LANES)
                            image = w[:, where] + far[:, k * LANES:(k + 1) * LANES]
                            w[:, where] = image
                            for m, other in enumerate(others):
                                accs[m] = accs[m] + other[:, where] * image
                            accs[-1] = accs[-1] + image * image
        return accs

    prepare_v()
    loads["rhs"].wait()

    def start_tile(t, acc):
        where = lanes_at(t, LANES)
        tile = rhs[:, where]
        xbf[:, where] = tile.astype(BF16)
        spread(tile, HALO + 2 * t)
        return acc + tile * tile

    norm = lax.fori_loop(0, width // LANES, start_tile, jnp.zeros((count, LANES), F32))
    pl.semaphore_wait(barrier, total - 1)
    first = operator(0, rhs, w_one, (rhs,))
    norm_sq, cross, image_sq = all_sum(0, [norm] + first)
    beta = jnp.sqrt(norm_sq)
    h11 = cross / norm_sq
    h21 = jnp.sqrt(image_sq / norm_sq - h11 * h11)
    scale = 1.0 / (beta * h21)

    def second_tile(t, carry):
        where = lanes_at(t, LANES)
        tile = (w_one[:, where] - h11 * rhs[:, where]) * scale
        q_two[:, where] = tile
        xbf[:, where] = tile.astype(BF16)
        spread(tile, HALO + 2 * t)
        return carry

    lax.fori_loop(0, width // LANES, second_tile, 0)
    second = operator(1, q_two, w_two, (rhs, q_two))
    with_first, h22, image_sq = all_sum(1, second)
    h12 = with_first / beta
    h32 = jnp.sqrt(image_sq - (h12 * h12 + h22 * h22))
    m11 = h11 * h11 + h21 * h21
    m12 = h11 * h12 + h21 * h22
    m22 = h12 * h12 + h22 * h22 + h32 * h32
    det = m11 * m22 - m12 * m12
    y1 = (m22 * h11 - m12 * h12) / det
    y2 = beta * (m11 * h12 - m12 * h11) / det

    def last_tile(t, carry):
        where = lanes_at(t, LANES)
        sol[:, where] = y1 * rhs[:, where] + y2 * q_two[:, where]
        res[:, where] = rhs[:, where] - y1 * w_one[:, where] - y2 * w_two[:, where]
        return carry

    lax.fori_loop(0, width // LANES, last_tile, 0)


def body(rhs, near_blocks, near_offsets, v_factor, mix_col, mix_row, u_factor):
    n_row = lax.axis_size("row")
    n_col = lax.axis_size("col")
    count, width = rhs.shape
    leaves, nnear = near_offsets.shape
    pieces = near_blocks.shape[2] // LANES
    near_rows = (
        near_blocks.reshape(leaves, nnear, pieces, LANES).transpose(0, 2, 1, 3).reshape(leaves * pieces * nnear, LANES)
    )
    mixc = mix_col[0]
    slots = leaves // n_col
    sub = slots // n_row
    total = n_row * n_col
    operands = (rhs, near_rows, v_factor, mixc, mix_row, u_factor)
    vmem = pltpu.VMEM
    dma = pltpu.SemaphoreType.DMA
    field = vmem((count, width), F32)
    hbm_spec = pl.BlockSpec(memory_space=pltpu.HBM)
    return pl.pallas_call(
        kernel,
        out_shape=(jax.ShapeDtypeStruct((count, width), F32),) * 2,
        in_specs=[pl.BlockSpec(memory_space=pltpu.SMEM)] + [hbm_spec] * 6,
        out_specs=(pl.BlockSpec(memory_space=pltpu.VMEM),) * 2,
        scratch_shapes=[
            field,
            vmem(near_rows.shape, BF16),
            vmem(v_factor.shape, BF16),
            vmem(mixc.shape, BF16),
            vmem(mix_row.shape, BF16),
            vmem(u_factor.shape, BF16),
            vmem((leaves * LEAF, nnear * LEAF), BF16),
            vmem((leaves * LEAF, LANES), BF16),
            vmem((leaves * RANK, 2 * LANES), BF16),
            vmem((nnear * LEAF, pieces * nnear), BF16),
            vmem((16 * LEAF, 256), BF16),
            vmem((16 * RANK, 256), BF16),
            vmem((count, width), BF16),
            vmem((leaves + 2 * HALO, count, LANES), BF16),
            field,
            field,
            field,
            vmem((n_col, count, slots * RANK), BF16),
            vmem((2, n_col, count, slots * RANK), BF16),
            vmem((n_row, sub, count, n_col * RANK), BF16),
            vmem((2, n_row, sub, count, n_col * RANK), BF16),
            vmem((2, 2, count, HALO * LEAF), BF16),
            vmem((2, 1, LANES), F32),
            vmem((2, total, 1, LANES), F32),
            dma((6,)),
            dma((2, 2)),
            dma((2, 2)),
            dma((2, n_col)),
            dma((2, n_col)),
            dma((2, n_row)),
            dma((2, n_row)),
            dma((2, total)),
            dma((2, total)),
        ],
        compiler_params=pltpu.CompilerParams(
            collective_id=0, has_side_effects=True, vmem_limit_bytes=34 * 1024 * 1024
        ),
        name="gmres",
    )(near_offsets, *(pltpu.with_memory_space_constraint(a, pltpu.HBM) for a in operands))


def solution(mesh):
    in_specs = (
        P(None, ("row", "col")),
        P(("row", "col"), None, None),
        P(("row", "col"), None),
        P(("row", "col"), None),
        P("row", "col", None, None),
        P("row", "col", None, None),
        P(("row", "col"), None),
    )
    out_specs = (P(None, ("row", "col")), P(None, ("row", "col")))
    return jax.shard_map(body, mesh=mesh, in_specs=in_specs, out_specs=out_specs, check_vma=False)
```

```python
import jax
import jax.numpy as jnp
from jax import lax
from jax.experimental import pallas as pl
from jax.experimental.pallas import tpu as pltpu
from jax.sharding import PartitionSpec as P

LEAF = 64
RANK = 32
HALO = 4
LANES = 128
QUAD = LANES // RANK
BF16 = jnp.bfloat16
F32 = jnp.float32
MESH = pl.DeviceIdType.MESH


def iota(shape, dim):
    return lax.broadcasted_iota(jnp.int32, shape, dim)


def dot(a, b):
    return jnp.dot(a, b, preferred_element_type=F32)


def lanes_at(index, width):
    return pl.ds(pl.multiple_of(index * width, width), width)


def regroup(tiles, group):
    out = []
    for j in range(QUAD):
        made = None
        for c in range(QUAD):
            shift = (c - j) * RANK % LANES
            moved = pltpu.roll(tiles[c], shift, 1) if shift else tiles[c]
            made = moved if made is None else jnp.where(group == c, moved, made)
        out.append(made)
    return out


def kernel(
    offs, rhs_h, near_h, v_h, mixc_h, mixr_h, u_h, sol, res,
    rhs, near_raw, v_raw, mixc, mixr, u_raw,
    near_w, v_big, u_big, pick_near, pick_v, pick_u, order,
    xbf, xdup, w_one, w_two, q_two,
    zbuf, zrecv, tbuf, trecv, halo, part, sums,
    load_sem, halo_s, halo_r, z_s, z_r, t_s, t_r, sum_s, sum_r,
):
    n_row = lax.axis_size("row")
    n_col = lax.axis_size("col")
    total = n_row * n_col
    row = lax.axis_index("row")
    col = lax.axis_index("col")
    me = row * n_col + col
    count, width = rhs.shape
    leaves = width // LEAF
    nnear = offs.shape[0]
    pieces = LEAF // 2
    slots = leaves // n_col
    sub = slots // n_row
    edge = HALO * LEAF

    loads = {}
    for at, (name, src, dst) in enumerate(
        (("v", v_h, v_raw), ("rhs", rhs_h, rhs), ("near", near_h, near_raw),
         ("mixc", mixc_h, mixc), ("mixr", mixr_h, mixr), ("u", u_h, u_raw))
    ):
        loads[name] = pltpu.make_async_copy(src, dst, load_sem.at[at])
        if name in ("v", "rhs"):
            loads[name].start()

    barrier = pltpu.get_barrier_semaphore()
    before = lax.rem(me + total - 1, total)
    after = lax.rem(me + 1, total)
    before_id = (before // n_col, lax.rem(before, n_col))
    after_id = (after // n_col, lax.rem(after, n_col))

    def col_id(step):
        return (row, lax.rem(col + step, n_col))

    def row_id(step):
        return (lax.rem(row + step, n_row), col)

    def any_id(step):
        other = lax.rem(me + step, total)
        return (other // n_col, lax.rem(other, n_col))

    def greet(step, carry):
        pl.semaphore_signal(barrier, inc=1, device_id=any_id(step), device_id_type=MESH)
        return carry

    lax.fori_loop(1, total, greet, 0)

    lane = iota((count, LANES), 1)
    low = lane < LEAF
    group = lane // RANK

    r = iota(pick_v.shape, 0)
    c = iota(pick_v.shape, 1)
    pick_v[...] = jnp.where((c % 16 == r // LEAF) & (c // 16 == r % LEAF // QUAD), 1.0, 0.0).astype(BF16)
    r = iota(pick_u.shape, 0)
    c = iota(pick_u.shape, 1)
    pick_u[...] = jnp.where((c % 16 == r // RANK) & (c // 16 == r % RANK // 2), 1.0, 0.0).astype(BF16)
    r = iota(pick_near.shape, 0)
    c = iota(pick_near.shape, 1)
    pick_near[...] = jnp.where((c % nnear == r // pieces) & (c // nnear == r % pieces), 1.0, 0.0).astype(BF16)

    r = iota(order.shape, 0) % LANES
    c = iota(order.shape, 1)
    order[...] = jnp.where(c == r // LEAF * LEAF + r % pieces * 2 + r % LEAF // pieces, 1.0, 0.0).astype(BF16)

    def prepare_v():
        loads["v"].wait()
        for name in ("near", "mixc", "mixr", "u"):
            loads[name].start()
        rr = iota((QUAD * LEAF, LANES), 0)
        gg = iota((QUAD * LEAF, LANES), 1) // RANK
        own = gg == rr % QUAD
        place = gg == rr // LEAF

        def block(b, carry):
            base = pl.multiple_of(b * 16, 16)
            rows = jnp.concatenate(
                [v_raw[pl.ds(base, 16), t * LANES:(t + 1) * LANES] for t in range(16)], axis=0
            )
            for q in range(4):
                size = QUAD * LEAF
                m = dot(pick_v[q * size:(q + 1) * size, :], rows)
                m = jnp.where(own, m, 0.0)
                m = m + pltpu.roll(m, RANK, 1)
                m = m + pltpu.roll(m, 2 * RANK, 1)
                at = pl.multiple_of(b * 16 * LEAF + q * size, size)
                v_big[pl.ds(at, size), :] = jnp.where(place, m, 0.0).astype(BF16)
            return carry

        lax.fori_loop(0, leaves // 16, block, 0)

    def prepare_u():
        loads["u"].wait()
        size = QUAD * RANK
        rr = iota((size, LANES), 0)
        half = iota((size, LANES), 1) // LEAF
        own = half == rr % 2
        place = (rr // RANK) - half

        def block(b, carry):
            base = pl.multiple_of(b * 16, 16)
            rows = jnp.concatenate(
                [u_raw[pl.ds(base, 16), t * LANES:(t + 1) * LANES] for t in range(16)], axis=0
            )
            for q in range(4):
                m = dot(pick_u[q * size:(q + 1) * size, :], rows)
                m = jnp.where(own, m, 0.0)
                m = m + pltpu.roll(m, LEAF, 1)
                at = pl.multiple_of(b * 16 * RANK + q * size, size)
                u_big[pl.ds(at, size), 0:LANES] = jnp.where(place == 0, m, 0.0).astype(BF16)
                u_big[pl.ds(at, size), LANES:2 * LANES] = jnp.where(place == 2, m, 0.0).astype(BF16)
            return carry

        lax.fori_loop(0, leaves // 16, block, 0)

    def prepare_near():
        loads["near"].wait()
        left = iota((pieces, LANES), 1) < LEAF
        size = nnear * LEAF // 2

        def block(b, carry):
            for k in range(2):
                twin = b * 4 + k * 2
                both = dot(
                    pick_near[...],
                    jnp.concatenate(
                        [near_raw[lanes_at(twin, size), :], near_raw[lanes_at(twin + 1, size), :]], axis=1
                    ),
                )
                for which in range(2):
                    m = both[:, which * LANES:(which + 1) * LANES]
                    for pair in range(nnear // 2):
                        a = m[2 * pair * pieces:(2 * pair + 1) * pieces]
                        d = m[(2 * pair + 1) * pieces:(2 * pair + 2) * pieces]
                        even = jnp.where(left, a, pltpu.roll(d, LEAF, 1))
                        odd = jnp.where(left, pltpu.roll(a, LEAF, 1), d)
                        for parity, made in ((0, even), (1, odd)):
                            near_w[
                                lanes_at((twin + which) * 2 + parity, pieces), pair * LANES:(pair + 1) * LANES
                            ] = made.astype(BF16)
            return carry

        lax.fori_loop(0, leaves // 4, block, 0)

    def spread(tile, first):
        turned = pltpu.roll(tile, LEAF, 1)
        xdup[first] = jnp.where(low, tile, turned).astype(BF16)
        xdup[first + 1] = jnp.where(low, turned, tile).astype(BF16)

    def remote(src, dst, send, recv, to):
        return pltpu.make_async_remote_copy(
            src_ref=src, dst_ref=dst, send_sem=send, recv_sem=recv, device_id=to, device_id_type=MESH
        )

    def all_sum(at, rows):
        spot = lane - iota((count, LANES), 0)
        spread_out = jnp.zeros((count, LANES), F32)
        for k, acc in enumerate(rows):
            spread_out = jnp.where(spot == k * count, jnp.sum(acc, axis=1, keepdims=True), spread_out)
        line = jnp.sum(spread_out, axis=0, keepdims=True)
        part[at] = line
        sums[at, 0] = line

        def copy(s):
            return remote(part.at[at], sums.at[at, s], sum_s.at[at, s], sum_r.at[at, s], any_id(s))

        def start(s, carry):
            copy(s).start()
            return carry

        def wait(s, carry):
            copy(s).wait()
            return carry

        lax.fori_loop(1, total, start, 0)
        lax.fori_loop(1, total, wait, 0)
        parts = [sums[at, lax.rem(me + total - d, total)] for d in range(total)]
        while len(parts) > 1:
            parts = [parts[i] + parts[i + 1] for i in range(0, len(parts), 2)]
        line = parts[0]
        return [
            jnp.sum(jnp.where(spot == k * count, line, 0.0), axis=1, keepdims=True) for k in range(len(rows))
        ]

    def operator(at, x, w, others):
        h_low = remote(xbf.at[:, width - edge:width], halo.at[at, 0], halo_s.at[at, 0], halo_r.at[at, 0], after_id)
        h_high = remote(xbf.at[:, 0:edge], halo.at[at, 1], halo_s.at[at, 1], halo_r.at[at, 1], before_id)
        h_low.start()
        h_high.start()
        tiles = slots // QUAD
        for g4 in range(leaves // QUAD):
            z = dot(xbf[:, g4 * 256:(g4 + 1) * 256], v_big[g4 * 256:(g4 + 1) * 256, :])
            zbuf[g4 // tiles, :, g4 % tiles * LANES:(g4 % tiles + 1) * LANES] = z.astype(BF16)
        z_copies = []
        for s in range(1, n_col):
            z_copies.append(
                remote(zbuf.at[lax.rem(col + s, n_col)], zrecv.at[at, s], z_s.at[at, s], z_r.at[at, s], col_id(s))
            )
            z_copies[-1].start()
        zrecv[at, 0] = zbuf[col]
        if at == 0:
            prepare_near()
        h_low.wait()
        h_high.wait()
        for side, beyond, first in ((0, me == 0, 0), (1, me == total - 1, leaves + HALO)):
            for k in range(HALO // 2):
                tile = halo[at, side, :, k * LANES:(k + 1) * LANES].astype(F32)
                spread(jnp.where(beyond, 0.0, tile), first + 2 * k)

        def near(b, carry):
            for pair in range(4):
                outs = []
                for k in range(2):
                    leaf = b * 8 + pair * 2 + k
                    picked = [xdup[leaf + HALO + offs[n, leaf]] for n in range(nnear)]
                    left = jnp.concatenate(
                        [jnp.where(low, picked[2 * m], picked[2 * m + 1]) for m in range(nnear // 2)], axis=1
                    )
                    outs.append(
                        lax.dot_general(
                            left, near_w[lanes_at(leaf, LEAF), :], (((1,), (1,)), ((), ())),
                            preferred_element_type=F32,
                        )
                    )
                where = lanes_at(b * 4 + pair, LANES)
                both = jnp.concatenate(outs, axis=1)
                high = both.astype(BF16)
                rest = (both - high.astype(F32)).astype(BF16)
                w[:, where] = x[:, where] + dot(jnp.concatenate([high, rest], axis=1), order[...])
            return carry

        steps = leaves // 8
        lax.fori_loop(0, steps // 2, near, 0)
        for copy in z_copies:
            copy.wait()
        if at == 0:
            loads["mixc"].wait()
        for jt in range(tiles):
            lefts = [[] for _ in range(QUAD)]
            for cq in range(n_col // QUAD):
                got = regroup(
                    [
                        zrecv[at, lax.rem(col + n_col - (cq * QUAD + c4), n_col), :, jt * LANES:(jt + 1) * LANES].astype(F32)
                        for c4 in range(QUAD)
                    ],
                    group,
                )
                for j4 in range(QUAD):
                    lefts[j4].append(got[j4].astype(BF16))
            for j4 in range(QUAD):
                j = jt * QUAD + j4
                first = dot(jnp.concatenate(lefts[j4], axis=1), mixc[j])
                tbuf[j // sub, j % sub] = first.astype(BF16)
        t_copies = []
        for s in range(1, n_row):
            t_copies.append(
                remote(tbuf.at[lax.rem(row + s, n_row)], trecv.at[at, s], t_s.at[at, s], t_r.at[at, s], row_id(s))
            )
            t_copies[-1].start()
        trecv[at, 0] = tbuf[row]
        if at == 0:
            prepare_u()
        lax.fori_loop(steps // 2, steps, near, 0)
        for copy in t_copies:
            copy.wait()
        if at == 0:
            loads["mixr"].wait()
        accs = [jnp.zeros((count, LANES), F32) for _ in range(len(others) + 1)]
        for i in range(sub):
            for pq in range(n_col // QUAD):
                lefts = [[] for _ in range(QUAD)]
                for rq in range(n_row // QUAD):
                    got = regroup(
                        [
                            trecv[at, lax.rem(row + n_row - (rq * QUAD + r4), n_row), i, :, pq * LANES:(pq + 1) * LANES].astype(F32)
                            for r4 in range(QUAD)
                        ],
                        group,
                    )
                    for p4 in range(QUAD):
                        lefts[p4].append(got[p4].astype(BF16))
                for p4 in range(QUAD):
                    p = pq * QUAD + p4
                    second = dot(jnp.concatenate(lefts[p4], axis=1), mixr[i, p]).astype(BF16)
                    for tt in range(n_row // QUAD):
                        at4 = (i * n_col + p) * (n_row // QUAD) + tt
                        far = dot(second[:, tt * LANES:(tt + 1) * LANES], u_big[at4 * LANES:(at4 + 1) * LANES, :])
                        for k in range(2):
                            where = slice(at4 * 256 + k * LANES, at4 * 256 + (k + 1) * LANES)
                            image = w[:, where] + far[:, k * LANES:(k + 1) * LANES]
                            w[:, where] = image
                            for m, other in enumerate(others):
                                accs[m] = accs[m] + other[:, where] * image
                            accs[-1] = accs[-1] + image * image
        return accs

    prepare_v()
    loads["rhs"].wait()

    def start_tile(t, acc):
        where = lanes_at(t, LANES)
        tile = rhs[:, where]
        xbf[:, where] = tile.astype(BF16)
        spread(tile, HALO + 2 * t)
        return acc + tile * tile

    norm = lax.fori_loop(0, width // LANES, start_tile, jnp.zeros((count, LANES), F32))
    pl.semaphore_wait(barrier, total - 1)
    first = operator(0, rhs, w_one, (rhs,))
    norm_sq, cross, image_sq = all_sum(0, [norm] + first)
    beta = jnp.sqrt(norm_sq)
    h11 = cross / norm_sq
    h21 = jnp.sqrt(image_sq / norm_sq - h11 * h11)
    scale = 1.0 / (beta * h21)

    def second_tile(t, carry):
        where = lanes_at(t, LANES)
        tile = (w_one[:, where] - h11 * rhs[:, where]) * scale
        q_two[:, where] = tile
        xbf[:, where] = tile.astype(BF16)
        spread(tile, HALO + 2 * t)
        return carry

    lax.fori_loop(0, width // LANES, second_tile, 0)
    second = operator(1, q_two, w_two, (rhs, q_two))
    with_first, h22, image_sq = all_sum(1, second)
    h12 = with_first / beta
    h32 = jnp.sqrt(image_sq - (h12 * h12 + h22 * h22))
    m11 = h11 * h11 + h21 * h21
    m12 = h11 * h12 + h21 * h22
    m22 = h12 * h12 + h22 * h22 + h32 * h32
    det = m11 * m22 - m12 * m12
    y1 = (m22 * h11 - m12 * h12) / det
    y2 = beta * (m11 * h12 - m12 * h11) / det

    def last_tile(t, carry):
        where = lanes_at(t, LANES)
        sol[:, where] = y1 * rhs[:, where] + y2 * q_two[:, where]
        res[:, where] = rhs[:, where] - y1 * w_one[:, where] - y2 * w_two[:, where]
        return carry

    lax.fori_loop(0, width // LANES, last_tile, 0)


def body(rhs, near_blocks, near_offsets, v_factor, mix_col, mix_row, u_factor):
    n_row = lax.axis_size("row")
    n_col = lax.axis_size("col")
    count, width = rhs.shape
    leaves, nnear = near_offsets.shape
    pieces = near_blocks.shape[2] // LANES
    near_rows = (
        near_blocks.reshape(leaves, nnear, pieces, LANES).transpose(0, 2, 1, 3).reshape(leaves * pieces * nnear, LANES)
    )
    mixc = mix_col[0]
    slots = leaves // n_col
    sub = slots // n_row
    total = n_row * n_col
    operands = (rhs, near_rows, v_factor, mixc, mix_row, u_factor)
    vmem = pltpu.VMEM
    dma = pltpu.SemaphoreType.DMA
    field = vmem((count, width), F32)
    hbm_spec = pl.BlockSpec(memory_space=pltpu.HBM)
    return pl.pallas_call(
        kernel,
        out_shape=(jax.ShapeDtypeStruct((count, width), F32),) * 2,
        in_specs=[pl.BlockSpec(memory_space=pltpu.SMEM)] + [hbm_spec] * 6,
        out_specs=(pl.BlockSpec(memory_space=pltpu.VMEM),) * 2,
        scratch_shapes=[
            field,
            vmem(near_rows.shape, BF16),
            vmem(v_factor.shape, BF16),
            vmem(mixc.shape, BF16),
            vmem(mix_row.shape, BF16),
            vmem(u_factor.shape, BF16),
            vmem((leaves * LEAF, nnear * LEAF), BF16),
            vmem((leaves * LEAF, LANES), BF16),
            vmem((leaves * RANK, 2 * LANES), BF16),
            vmem((nnear * pieces, pieces * nnear), BF16),
            vmem((16 * LEAF, 256), BF16),
            vmem((16 * RANK, 256), BF16),
            vmem((2 * LANES, LANES), BF16),
            vmem((count, width), BF16),
            vmem((leaves + 2 * HALO, count, LANES), BF16),
            field,
            field,
            field,
            vmem((n_col, count, slots * RANK), BF16),
            vmem((2, n_col, count, slots * RANK), BF16),
            vmem((n_row, sub, count, n_col * RANK), BF16),
            vmem((2, n_row, sub, count, n_col * RANK), BF16),
            vmem((2, 2, count, HALO * LEAF), BF16),
            vmem((2, 1, LANES), F32),
            vmem((2, total, 1, LANES), F32),
            dma((6,)),
            dma((2, 2)),
            dma((2, 2)),
            dma((2, n_col)),
            dma((2, n_col)),
            dma((2, n_row)),
            dma((2, n_row)),
            dma((2, total)),
            dma((2, total)),
        ],
        compiler_params=pltpu.CompilerParams(
            collective_id=0, has_side_effects=True, vmem_limit_bytes=34 * 1024 * 1024
        ),
        name="gmres",
    )(near_offsets.T, *(pltpu.with_memory_space_constraint(a, pltpu.HBM) for a in operands))


def solution(mesh):
    in_specs = (
        P(None, ("row", "col")),
        P(("row", "col"), None, None),
        P(("row", "col"), None),
        P(("row", "col"), None),
        P("row", "col", None, None),
        P("row", "col", None, None),
        P(("row", "col"), None),
    )
    out_specs = (P(None, ("row", "col")), P(None, ("row", "col")))
    return jax.shard_map(body, mesh=mesh, in_specs=in_specs, out_specs=out_specs, check_vma=False)
```
